32 devices in a mesh: rep: 2 (over x), dp: 16 (over y, z, core).
Axes of the slice: x: 2, y: 2, z: 4, core: 2. Of those that a mesh axis runs over, the one named last changes fastest.
Arguments:
- g_w_gate: bfloat16 [32, 2, 1280, 3072], P(('rep', 'dp')), parts along dimension 0
- g_w_up: bfloat16 [32, 2, 1280, 3072], P(('rep', 'dp')), parts along dimension 0
- g_w_down: bfloat16 [32, 2, 3072, 1280], P(('rep', 'dp')), parts along dimension 0
- w_gate: bfloat16 [2, 1280, 3072], replicated
- w_up: bfloat16 [2, 1280, 3072], replicated
- w_down: bfloat16 [2, 3072, 1280], replicated
- m_w_gate: float32 [2, 1280, 3072], P(None, 'dp')
- m_w_up: float32 [2, 1280, 3072], P(None, 'dp')
- m_w_down: float32 [2, 3072, 1280], P(None, 'dp')
- v_w_gate: float32 [2, 1280, 3072], P(None, 'dp')
- v_w_up: float32 [2, 1280, 3072], P(None, 'dp')
- v_w_down: float32 [2, 3072, 1280], P(None, 'dp')
Outputs:
- output 1: bfloat16 [4, 1280, 3072], P('rep'), parts along dimension 0
- output 2: bfloat16 [4, 1280, 3072], P('rep'), parts along dimension 0
- output 3: bfloat16 [4, 3072, 1280], P('rep'), parts along dimension 0
- output 4: float32 [4, 1280, 3072], P('rep', 'dp'), parts along dimension 0
- output 5: float32 [4, 1280, 3072], P('rep', 'dp'), parts along dimension 0
- output 6: float32 [4, 3072, 1280], P('rep', 'dp'), parts along dimension 0
- output 7: float32 [4, 1280, 3072], P('rep', 'dp'), parts along dimension 0
- output 8: float32 [4, 1280, 3072], P('rep', 'dp'), parts along dimension 0
- output 9: float32 [4, 3072, 1280], P('rep', 'dp'), parts along dimension 0
There are 2 independent parts. The reference program is written for one: setup_inputs(seed, part) draws one part's arguments, and reference() takes and returns one part's arrays. A program takes and returns all parts, laid end to end along the dimension named above; an argument that names none is the same for every part.
All inputs are finite; a program needn't handle non-finite values.
Results may differ from the reference program's by a relative error of at most 0.022.
Values are sent between devices in bfloat16 or wider.
A program may use at most 2 GiB of HBM per device.

```python
import jax
import jax.numpy as jnp
from jax import lax

DEVICES = 16
D = 1280
FF = 3072
LAYERS = 2
NAMES = ("w_gate", "w_up", "w_down")
SHAPES = {"w_gate": (LAYERS, D, FF), "w_up": (LAYERS, D, FF), "w_down": (LAYERS, FF, D)}


def setup_inputs(seed: int = 0, part: int = 0) -> dict:
    kz, *keys = jax.random.split(jax.random.key(seed), 1 + 5 * len(NAMES))
    loud = 2.0 ** jax.random.uniform(kz, (), jnp.float32, -1.0, 1.0)
    drawn = {}
    for name, key, both in zip(NAMES, keys[:3], keys[3:6], strict=True):
        own = jax.random.normal(jax.random.fold_in(key, part), (DEVICES, *SHAPES[name]), jnp.float32)
        shared = jax.random.normal(jax.random.fold_in(both, part), SHAPES[name], jnp.float32)
        drawn["g_" + name] = (loud * (0.7 * shared / DEVICES + 0.7 * own * DEVICES**-0.5)).astype(jnp.bfloat16)
    for name, key in zip(NAMES, keys[6:9], strict=True):
        drawn[name] = (jax.random.normal(key, SHAPES[name], jnp.float32) * SHAPES[name][1] ** -0.5).astype(jnp.bfloat16)
    for name, key in zip(NAMES, keys[9:12], strict=True):
        drawn["m_" + name] = loud * 0.5 * jax.random.normal(key, SHAPES[name], jnp.float32)
    for name, key in zip(NAMES, keys[12:15], strict=True):
        drawn["v_" + name] = loud * loud * jax.random.uniform(key, SHAPES[name], jnp.float32, 0.5, 1.5)
    return drawn


def adamw(w, m, v, g):
    m = 0.9 * m + 0.1 * g
    v = 0.95 * v + 0.05 * g * g
    step = m * lax.rsqrt(v + 1e-8) + 0.1 * w
    return (w - 0.02 * step).astype(jnp.bfloat16), m, v


def clipped(gradients, sum_of_squares, count):
    factor = jnp.minimum(1.0, 0.5 * lax.rsqrt(sum_of_squares / count + 1e-30))
    return [g * factor for g in gradients]


def reference(g_w_gate, g_w_up, g_w_down, w_gate, w_up, w_down, m_w_gate, m_w_up, m_w_down, v_w_gate, v_w_up, v_w_down):
    def total(terms):
        return lax.scan(lambda so_far, term: (so_far + term.astype(jnp.float32), None), jnp.zeros(terms.shape[1:], jnp.float32), terms)[0]

    gradients = [total(terms).astype(jnp.bfloat16).astype(jnp.float32) for terms in (g_w_gate, g_w_up, g_w_down)]
    gradients = clipped(gradients, sum(jnp.sum(g * g) for g in gradients), sum(g.size for g in gradients))
    new = [
        adamw(w.astype(jnp.float32), m, v, g)
        for w, m, v, g in zip((w_gate, w_up, w_down), (m_w_gate, m_w_up, m_w_down), (v_w_gate, v_w_up, v_w_down), gradients, strict=True)
    ]
    return tuple(one[which] for which in range(3) for one in new)
```

```python
import functools

import jax
import jax.numpy as jnp
from jax import lax
from jax.experimental import pallas as pl
from jax.experimental.pallas import tpu as pltpu
from jax.sharding import PartitionSpec as P

MESH = pl.DeviceIdType.MESH
CHIPS, DEVICES = 8, 16
PIECES = [(i, way) for i in range(3) for way in range(2)]


def adamw(w, m, v, g):
    m = 0.9 * m + 0.1 * g
    v = 0.95 * v + 0.05 * g * g
    step = m * lax.rsqrt(v + 1e-8) + 0.1 * w
    return (w - 0.02 * step).astype(jnp.bfloat16), m, v


def at(place):
    return place + lax.div(place, 4) * (11 - 2 * place)


def tiles(height, width):
    wide = 512 if width % 512 == 0 else 640
    return height // 16, [slice(k, k + wide) for k in range(0, width, wide)]


def kernel(count, g, w, m, v, whole, new_m, new_v, held, squares, own_sem, m_sem, v_sem, ring_send, ring_recv, pair_send, pair_recv, sq_send, sq_recv):
    rep, me = lax.axis_index("rep"), lax.axis_index("dp")
    chip, core = lax.div(me, 2), lax.rem(me, 2)
    place = at(chip)
    heights = [one.shape[1] for one in new_m]
    slots = [held[0].at[0], held[0].at[1], held[0].at[2], held[0].at[3], held[1].at[0], held[1].at[1]]

    def device(place, core):
        return 2 * at(lax.rem(place + 2 * CHIPS, CHIPS)) + core

    def block(way, step):
        return place - 1 - step if way == 0 else place + 1 + step

    def rows(i, owner):
        return pl.ds(pl.multiple_of(owner * heights[i], 16), heights[i])

    def ring(j, step, owner):
        i, way = PIECES[j]
        part = whole[i].at[way, rows(i, owner)]
        return pltpu.make_async_remote_copy(
            src_ref=part, dst_ref=part, send_sem=ring_send.at[step, j], recv_sem=ring_recv.at[step, j],
            device_id=(rep, device(place + 1 if way == 0 else place - 1, core)), device_id_type=MESH,
        )

    def pair(j, step, source, owner):
        i, way = PIECES[j]
        return pltpu.make_async_remote_copy(
            src_ref=source, dst_ref=whole[i].at[way, rows(i, owner)], send_sem=pair_send.at[step, j], recv_sem=pair_recv.at[step, j],
            device_id=(rep, 2 * chip + 1 - core), device_id_type=MESH,
        )

    def term(j, step):
        i, way = PIECES[j]
        owner = device(block(way, step), 1 - core)
        return pair(j, step, g[i].at[0, way, rows(i, owner)], owner)

    def own(j, step):
        i, way = PIECES[j]
        return pltpu.make_async_copy(g[i].at[0, way, rows(i, device(block(way, step), core))], slots[j], own_sem.at[j])

    def load_w(j):
        i, way = PIECES[j]
        return pltpu.make_async_copy(w[i].at[way, rows(i, me)], slots[j], own_sem.at[j])

    def load_m(j):
        i, way = PIECES[j]
        return pltpu.make_async_copy(m[i].at[way], new_m[i].at[way], m_sem.at[j])

    def load_v(j):
        i, way = PIECES[j]
        return pltpu.make_async_copy(v[i].at[way], new_v[i].at[way], v_sem.at[j])

    def add(j, step, first=False):
        i, way = PIECES[j]
        groups, columns = tiles(heights[i], whole[i].shape[2])
        mine = pl.multiple_of(device(block(way, step), core) * heights[i], 16)
        other = pl.multiple_of(device(block(way, step), 1 - core) * heights[i], 16)

        def group(r, _):
            for c in columns:
                total = slots[j][pl.ds(r * 16, 16), c].astype(jnp.float32) + whole[i][way, pl.ds(mine + r * 16, 16), c].astype(jnp.float32)
                if not first:
                    total = total + whole[i][way, pl.ds(other + r * 16, 16), c].astype(jnp.float32)
                whole[i][way, pl.ds(other + r * 16, 16), c] = total.astype(jnp.bfloat16)
            return 0

        lax.fori_loop(0, groups, group, 0)

    def last_add(j, so_far):
        i, way = PIECES[j]
        groups, columns = tiles(heights[i], whole[i].shape[2])
        mine = pl.multiple_of(me * heights[i], 16)
        other = pl.multiple_of((2 * chip + 1 - core) * heights[i], 16)

        def group(r, so_far):
            for c in columns:
                total = slots[j][pl.ds(r * 16, 16), c].astype(jnp.float32) + whole[i][way, pl.ds(mine + r * 16, 16), c].astype(jnp.float32)
                total = (total + whole[i][way, pl.ds(other + r * 16, 16), c].astype(jnp.float32)).astype(jnp.bfloat16)
                whole[i][way, pl.ds(mine + r * 16, 16), c] = total
                total = total.astype(jnp.float32)
                total = total * total
                for k in range(0, total.shape[1], 128):
                    so_far = so_far + total[:8, k : k + 128] + total[8:, k : k + 128]
            return so_far

        return lax.fori_loop(0, groups, group, so_far)

    def update(j, factor):
        i, way = PIECES[j]
        groups, columns = tiles(heights[i], whole[i].shape[2])
        mine = pl.multiple_of(me * heights[i], 16)

        def group(r, _):
            for c in columns:
                here = (way, pl.ds(r * 16, 16), c)
                there = (way, pl.ds(mine + r * 16, 16), c)
                gradient = whole[i][there].astype(jnp.float32) * factor
                new, new_m[i][here], new_v[i][here] = adamw(slots[j][pl.ds(r * 16, 16), c].astype(jnp.float32), new_m[i][here], new_v[i][here], gradient)
                whole[i][there] = new
            return 0

        lax.fori_loop(0, groups, group, 0)

    every = range(len(PIECES))
    for j in every:
        own(j, 0).start()
    barrier = pltpu.get_barrier_semaphore()
    for k in range(1, DEVICES):
        pl.semaphore_signal(barrier, inc=1, device_id=(rep, lax.rem(me + k, DEVICES)), device_id_type=MESH)
    pl.semaphore_wait(barrier, DEVICES - 1)

    for step in range(2):
        for j in every:
            term(j, step).start()
    for j in every:
        own(j, 0).wait()
        term(j, 0).wait_recv()
        add(j, 0, first=True)
        ring(j, 0, device(block(PIECES[j][1], 0), 1 - core)).start()
        own(j, 1).start()
    for j in every:
        load_m(j).start()
        load_v(j).start()

    def reduce_step(step, _):
        for j in every:
            term(j, step + 1).start()
        for j in every:
            owner = device(block(PIECES[j][1], step), 1 - core)
            own(j, step).wait()
            term(j, step).wait_recv()
            ring(j, step - 1, owner).wait_recv()
            add(j, step)
            ring(j, step, owner).start()
            own(j, step + 1).start()
            ring(j, step - 1, owner).wait_send()
            term(j, step - 1).wait_send()
        return 0

    lax.fori_loop(1, CHIPS - 1, reduce_step, 0)

    so_far = jnp.zeros((8, 128), jnp.float32)
    for j in every:
        own(j, CHIPS - 1).wait()
        term(j, CHIPS - 1).wait_recv()
        ring(j, CHIPS - 2, 2 * chip + 1 - core).wait_recv()
        so_far = last_add(j, so_far)
        load_w(j).start()
    for j in every:
        term(j, CHIPS - 2).wait_send()
        term(j, CHIPS - 1).wait_send()
        ring(j, CHIPS - 2, 2 * chip + 1 - core).wait_send()

    squares[me] = so_far

    def tell(k):
        return pltpu.make_async_remote_copy(
            src_ref=squares.at[me], dst_ref=squares.at[me], send_sem=sq_send.at[k], recv_sem=sq_recv.at[k],
            device_id=(rep, lax.rem(me + k, DEVICES)), device_id_type=MESH,
        )

    for k in range(1, DEVICES):
        tell(k).start()
    for j in every:
        load_m(j).wait()
        load_v(j).wait()
        load_w(j).wait()
    for k in range(1, DEVICES):
        tell(k).wait_recv()
    total = squares[0]
    for k in range(1, DEVICES):
        total = total + squares[k]
    total = jnp.sum(jnp.sum(total, axis=0, keepdims=True), axis=1, keepdims=True)
    factor = jnp.minimum(1.0, 0.5 * lax.rsqrt(total / count + 1e-30))

    def carried(j, step):
        return device(place - step if PIECES[j][1] == 0 else place + step, core)

    def on(j, step):
        return ring(j, step, carried(j, step))

    def across(j, step):
        i, way = PIECES[j]
        owner = carried(j, step)
        return pair(j, step, whole[i].at[way, rows(i, owner)], owner)

    for j in every:
        update(j, factor)
        on(j, 0).start()
        across(j, 0).start()

    def gather_step(step, _):
        for j in every:
            on(j, step - 1).wait_recv()
            on(j, step).start()
            across(j, step).start()
            on(j, step - 1).wait_send()
            across(j, step - 1).wait_send()
        return 0

    lax.fori_loop(1, CHIPS - 1, gather_step, 0)
    for j in every:
        on(j, CHIPS - 2).wait_recv()
        across(j, CHIPS - 1).start()
        on(j, CHIPS - 2).wait_send()
        across(j, CHIPS - 2).wait_send()
    for k in range(1, DEVICES):
        tell(k).wait_send()
    for j in every:
        across(j, CHIPS - 1).wait_send()

    def arrived(step, _):
        for j in every:
            across(j, step).wait_recv()
        return 0

    lax.fori_loop(0, CHIPS, arrived, 0)


def put_out(*refs):
    copies = [pltpu.make_async_copy(refs[k].at[layer], refs[9 + k].at[layer], refs[18].at[k, layer]) for k in range(9) for layer in range(2)]
    for copy in copies:
        copy.start()
    for copy in copies:
        copy.wait()


def body(count, *refs):
    groups = [refs[k : k + 3] for k in range(0, 21, 3)]
    kernel(count, *groups, refs[21:23], *refs[23:])


def solution(mesh):
    def step(*arrays):
        weights, moments = arrays[3:6], arrays[6:9]
        count = DEVICES * sum(one.size for one in moments)
        heights = [one.shape[1] for one in moments]
        widths = [one.shape[2] for one in moments]
        dma = pltpu.SemaphoreType.DMA
        out = [pltpu.VMEM(one.shape, jnp.bfloat16) for one in weights] + 2 * [pltpu.VMEM(one.shape, jnp.float32) for one in moments]
        done = pl.pallas_call(
            functools.partial(body, count),
            out_shape=out,
            in_specs=[pl.BlockSpec(memory_space=pltpu.HBM)] * 12,
            out_specs=[pl.BlockSpec(memory_space=pltpu.VMEM)] * 9,
            scratch_shapes=[
                pltpu.VMEM((4, heights[0], widths[0]), jnp.bfloat16),
                pltpu.VMEM((2, heights[2], widths[2]), jnp.bfloat16),
                pltpu.VMEM((DEVICES, 8, 128), jnp.float32),
                dma((6,)), dma((6,)), dma((6,)),
                dma((7, 6)), dma((7, 6)), dma((8, 6)), dma((8, 6)),
                dma((DEVICES,)), dma((DEVICES,)),
            ],
            compiler_params=pltpu.CompilerParams(collective_id=0, has_side_effects=True, vmem_limit_bytes=4 << 20),
            name="train_step",
        )(*arrays)
        return pl.pallas_call(
            put_out,
            out_shape=[jax.ShapeDtypeStruct(one.shape, one.dtype) for one in done],
            in_specs=[pl.BlockSpec(memory_space=pltpu.VMEM)] * 9,
            out_specs=[pl.BlockSpec(memory_space=pltpu.HBM)] * 9,
            scratch_shapes=[dma((9, 2))],
            compiler_params=pltpu.CompilerParams(vmem_limit_bytes=1 << 20),
            name="put_out",
        )(*[pltpu.with_memory_space_constraint(one, pltpu.VMEM) for one in done])

    all_of, cut = P(None, None, None), P(None, "dp", None)
    return jax.shard_map(
        step,
        mesh=mesh,
        in_specs=(P(("rep", "dp"), None, None, None),) * 3 + (all_of,) * 3 + (cut,) * 6,
        out_specs=(P("rep", None, None),) * 3 + (P("rep", "dp", None),) * 6,
        check_vma=False,
    )
```

```python
import functools

import jax
import jax.numpy as jnp
from jax import lax
from jax.experimental import pallas as pl
from jax.experimental.pallas import tpu as pltpu
from jax.sharding import PartitionSpec as P

MESH = pl.DeviceIdType.MESH
CHIPS, DEVICES = 8, 16
PIECES = [(i, way) for i in range(3) for way in range(2)]


def adamw(w, m, v, g):
    m = 0.9 * m + 0.1 * g
    v = 0.95 * v + 0.05 * g * g
    step = m * lax.rsqrt(v + 1e-8) + 0.1 * w
    return (w - 0.02 * step).astype(jnp.bfloat16), m, v


def at(place):
    return place + lax.div(place, 4) * (11 - 2 * place)


def tiles(height, width):
    wide = 512 if width % 512 == 0 else 640
    return height // 16, [slice(k, k + wide) for k in range(0, width, wide)]


def kernel(count, g, w, m, v, whole, new_m, new_v, held, squares, own_sem, m_sem, v_sem, ring_send, ring_recv, pair_send, pair_recv, sq_send, sq_recv):
    rep, me = lax.axis_index("rep"), lax.axis_index("dp")
    chip, core = lax.div(me, 2), lax.rem(me, 2)
    place = at(chip)
    heights = [one.shape[1] for one in new_m]
    slots = [held[0].at[0], held[0].at[1], held[0].at[2], held[0].at[3], held[1].at[0], held[1].at[1]]

    def device(place, core):
        return 2 * at(lax.rem(place + 2 * CHIPS, CHIPS)) + core

    def block(way, step):
        return place - 1 - step if way == 0 else place + 1 + step

    def rows(i, owner):
        return pl.ds(pl.multiple_of(owner * heights[i], 16), heights[i])

    def ring(j, step, owner):
        i, way = PIECES[j]
        part = whole[i].at[way, rows(i, owner)]
        return pltpu.make_async_remote_copy(
            src_ref=part, dst_ref=part, send_sem=ring_send.at[step, j], recv_sem=ring_recv.at[step, j],
            device_id=(rep, device(place + 1 if way == 0 else place - 1, core)), device_id_type=MESH,
        )

    def pair(j, step, source, owner):
        i, way = PIECES[j]
        return pltpu.make_async_remote_copy(
            src_ref=source, dst_ref=whole[i].at[way, rows(i, owner)], send_sem=pair_send.at[step, j], recv_sem=pair_recv.at[step, j],
            device_id=(rep, 2 * chip + 1 - core), device_id_type=MESH,
        )

    def term(j, step):
        i, way = PIECES[j]
        owner = device(block(way, step), 1 - core)
        return pair(j, step, g[i].at[0, way, rows(i, owner)], owner)

    def own(j, step):
        i, way = PIECES[j]
        return pltpu.make_async_copy(g[i].at[0, way, rows(i, device(block(way, step), core))], slots[j], own_sem.at[j])

    def load_w(j):
        i, way = PIECES[j]
        return pltpu.make_async_copy(w[i].at[way, rows(i, me)], slots[j], own_sem.at[j])

    def load_m(j):
        i, way = PIECES[j]
        return pltpu.make_async_copy(m[i].at[way], new_m[i].at[way], m_sem.at[j])

    def load_v(j):
        i, way = PIECES[j]
        return pltpu.make_async_copy(v[i].at[way], new_v[i].at[way], v_sem.at[j])

    def add(j, step, first=False):
        i, way = PIECES[j]
        groups, columns = tiles(heights[i], whole[i].shape[2])
        mine = pl.multiple_of(device(block(way, step), core) * heights[i], 16)
        other = pl.multiple_of(device(block(way, step), 1 - core) * heights[i], 16)

        def group(r, _):
            for c in columns:
                total = slots[j][pl.ds(r * 16, 16), c].astype(jnp.float32) + whole[i][way, pl.ds(mine + r * 16, 16), c].astype(jnp.float32)
                if not first:
                    total = total + whole[i][way, pl.ds(other + r * 16, 16), c].astype(jnp.float32)
                whole[i][way, pl.ds(other + r * 16, 16), c] = total.astype(jnp.bfloat16)
            return 0

        lax.fori_loop(0, groups, group, 0)

    def last_add(j, so_far):
        i, way = PIECES[j]
        groups, columns = tiles(heights[i], whole[i].shape[2])
        mine = pl.multiple_of(me * heights[i], 16)
        other = pl.multiple_of((2 * chip + 1 - core) * heights[i], 16)

        def group(r, so_far):
            for c in columns:
                total = slots[j][pl.ds(r * 16, 16), c].astype(jnp.float32) + whole[i][way, pl.ds(mine + r * 16, 16), c].astype(jnp.float32)
                total = (total + whole[i][way, pl.ds(other + r * 16, 16), c].astype(jnp.float32)).astype(jnp.bfloat16)
                whole[i][way, pl.ds(mine + r * 16, 16), c] = total
                total = total.astype(jnp.float32)
                total = total * total
                for k in range(0, total.shape[1], 128):
                    so_far = so_far + total[:8, k : k + 128] + total[8:, k : k + 128]
            return so_far

        return lax.fori_loop(0, groups, group, so_far)

    def update(j, factor):
        i, way = PIECES[j]
        groups, columns = tiles(heights[i], whole[i].shape[2])
        mine = pl.multiple_of(me * heights[i], 16)

        def group(r, _):
            for c in columns:
                here = (way, pl.ds(r * 16, 16), c)
                there = (way, pl.ds(mine + r * 16, 16), c)
                gradient = whole[i][there].astype(jnp.float32) * factor
                new, new_m[i][here], new_v[i][here] = adamw(slots[j][pl.ds(r * 16, 16), c].astype(jnp.float32), new_m[i][here], new_v[i][here], gradient)
                whole[i][there] = new
            return 0

        lax.fori_loop(0, groups, group, 0)

    every = range(len(PIECES))
    for j in every:
        own(j, 0).start()
    barrier = pltpu.get_barrier_semaphore()
    for k in range(1, DEVICES):
        pl.semaphore_signal(barrier, inc=1, device_id=(rep, lax.rem(me + k, DEVICES)), device_id_type=MESH)
    pl.semaphore_wait(barrier, DEVICES - 1)

    for step in range(2):
        for j in every:
            term(j, step).start()
    for j in every:
        own(j, 0).wait()
        term(j, 0).wait_recv()
        add(j, 0, first=True)
        ring(j, 0, device(block(PIECES[j][1], 0), 1 - core)).start()
        own(j, 1).start()
    for j in every:
        load_m(j).start()
        load_v(j).start()

    def reduce_step(step, _):
        for j in every:
            term(j, step + 1).start()
        for j in every:
            owner = device(block(PIECES[j][1], step), 1 - core)
            own(j, step).wait()
            term(j, step).wait_recv()
            ring(j, step - 1, owner).wait_recv()
            add(j, step)
            ring(j, step, owner).start()
            own(j, step + 1).start()
            ring(j, step - 1, owner).wait_send()
            term(j, step - 1).wait_send()
        return 0

    lax.fori_loop(1, CHIPS - 1, reduce_step, 0)

    so_far = jnp.zeros((8, 128), jnp.float32)
    for j in every:
        own(j, CHIPS - 1).wait()
        term(j, CHIPS - 1).wait_recv()
        ring(j, CHIPS - 2, 2 * chip + 1 - core).wait_recv()
        so_far = last_add(j, so_far)
        load_w(j).start()
    for j in every:
        term(j, CHIPS - 2).wait_send()
        term(j, CHIPS - 1).wait_send()
        ring(j, CHIPS - 2, 2 * chip + 1 - core).wait_send()

    squares[me] = so_far

    def tell(k):
        return pltpu.make_async_remote_copy(
            src_ref=squares.at[me], dst_ref=squares.at[me], send_sem=sq_send.at[k], recv_sem=sq_recv.at[k],
            device_id=(rep, lax.rem(me + k, DEVICES)), device_id_type=MESH,
        )

    for k in range(1, DEVICES):
        tell(k).start()
    for j in every:
        load_m(j).wait()
        load_v(j).wait()
        load_w(j).wait()
    for k in range(1, DEVICES):
        tell(k).wait_recv()
    total = squares[0]
    for k in range(1, DEVICES):
        total = total + squares[k]
    total = jnp.sum(jnp.sum(total, axis=0, keepdims=True), axis=1, keepdims=True)
    factor = jnp.minimum(1.0, 0.5 * lax.rsqrt(total / count + 1e-30))

    def carried(j, step):
        return device(place - step if PIECES[j][1] == 0 else place + step, core)

    def on(j, step):
        return ring(j, step, carried(j, step))

    def across(j, step):
        i, way = PIECES[j]
        owner = carried(j, step)
        return pair(j, step, whole[i].at[way, rows(i, owner)], owner)

    for j in every:
        update(j, factor)
        on(j, 0).start()
        across(j, 0).start()

    def gather_step(step, _):
        for j in every:
            on(j, step - 1).wait_recv()
            on(j, step).start()
            across(j, step).start()
            on(j, step - 1).wait_send()
            across(j, step - 1).wait_send()
        return 0

    lax.fori_loop(1, CHIPS - 1, gather_step, 0)
    for j in every:
        on(j, CHIPS - 2).wait_recv()
        across(j, CHIPS - 1).start()
        on(j, CHIPS - 2).wait_send()
        across(j, CHIPS - 2).wait_send()
    for k in range(1, DEVICES):
        tell(k).wait_send()
    for j in every:
        across(j, CHIPS - 1).wait_send()

    def arrived(step, _):
        for j in every:
            across(j, step).wait_recv()
        return 0

    lax.fori_loop(0, CHIPS, arrived, 0)


def put_out(*refs):
    copies = [pltpu.make_async_copy(refs[k].at[layer], refs[9 + k].at[layer], refs[18].at[k, layer]) for k in range(9) for layer in range(2)]
    for copy in copies:
        copy.start()
    for copy in copies:
        copy.wait()


def body(count, *refs):
    groups = [refs[k : k + 3] for k in range(0, 21, 3)]
    kernel(count, *groups, refs[21:23], *refs[23:])


def solution(mesh):
    def step(*arrays):
        weights, moments = arrays[3:6], arrays[6:9]
        count = DEVICES * sum(one.size for one in moments)
        heights = [one.shape[1] for one in moments]
        widths = [one.shape[2] for one in moments]
        dma = pltpu.SemaphoreType.DMA
        out = [pltpu.VMEM(one.shape, jnp.bfloat16) for one in weights] + 2 * [pltpu.VMEM(one.shape, jnp.float32) for one in moments]
        done = pl.pallas_call(
            functools.partial(body, count),
            out_shape=out,
            in_specs=[pl.BlockSpec(memory_space=pltpu.HBM)] * 12,
            out_specs=[pl.BlockSpec(memory_space=pltpu.VMEM)] * 9,
            scratch_shapes=[
                pltpu.VMEM((4, heights[0], widths[0]), jnp.bfloat16),
                pltpu.VMEM((2, heights[2], widths[2]), jnp.bfloat16),
                pltpu.VMEM((DEVICES, 8, 128), jnp.float32),
                dma((6,)), dma((6,)), dma((6,)),
                dma((7, 6)), dma((7, 6)), dma((8, 6)), dma((8, 6)),
                dma((DEVICES,)), dma((DEVICES,)),
            ],
            compiler_params=pltpu.CompilerParams(collective_id=0, has_side_effects=True, vmem_limit_bytes=4 << 20),
            name="train_step",
        )(*arrays)
        return pl.pallas_call(
            put_out,
            out_shape=[jax.ShapeDtypeStruct(one.shape, one.dtype) for one in done],
            in_specs=[pl.BlockSpec(memory_space=pltpu.VMEM)] * 9,
            out_specs=[pl.BlockSpec(memory_space=pltpu.HBM)] * 9,
            scratch_shapes=[dma((9, 2))],
            compiler_params=pltpu.CompilerParams(vmem_limit_bytes=4 << 20),
            name="put_out",
        )(*[pltpu.with_memory_space_constraint(one, pltpu.VMEM) for one in done])

    all_of, cut = P(None, None, None), P(None, "dp", None)
    return jax.shard_map(
        step,
        mesh=mesh,
        in_specs=(P(("rep", "dp"), None, None, None),) * 3 + (all_of,) * 3 + (cut,) * 6,
        out_specs=(P("rep", None, None),) * 3 + (P("rep", "dp", None),) * 6,
        check_vma=False,
    )
```

```python
import functools

import jax
import jax.numpy as jnp
from jax import lax
from jax.experimental import pallas as pl
from jax.experimental.pallas import tpu as pltpu
from jax.sharding import PartitionSpec as P

MESH = pl.DeviceIdType.MESH
CHIPS, DEVICES = 8, 16
FIRST = ((0, 2), (2, 5))
ORDER = [(0, FIRST[0]), (1, FIRST[0]), (0, FIRST[1]), (1, FIRST[1]), (2, None), (3, None), (4, None), (5, None)]
PIECES = [(i, way) for i in range(3) for way in range(2)]


def adamw(w, m, v, g):
    m = 0.9 * m + 0.1 * g
    v = 0.95 * v + 0.05 * g * g
    step = m * lax.rsqrt(v + 1e-8) + 0.1 * w
    return (w - 0.02 * step).astype(jnp.bfloat16), m, v


def at(place):
    return place + lax.div(place, 4) * (11 - 2 * place)


def tiles(height, width):
    wide = 512 if width % 512 == 0 else 640
    return height // 16, [slice(k, k + wide) for k in range(0, width, wide)]


def kernel(count, g, w, m, v, whole, new_m, new_v, held, squares, own_sem, m_sem, v_sem, ring_send, ring_recv, pair_send, pair_recv, sq_send, sq_recv):
    rep, me = lax.axis_index("rep"), lax.axis_index("dp")
    chip, core = lax.div(me, 2), lax.rem(me, 2)
    place = at(chip)
    heights = [one.shape[1] for one in new_m]
    slots = [held[0].at[0], held[0].at[1], held[0].at[2], held[0].at[3], held[1].at[0], held[1].at[1]]

    def device(place, core):
        return 2 * at(lax.rem(place + 2 * CHIPS, CHIPS)) + core

    def block(way, step):
        return place - 1 - step if way == 0 else place + 1 + step

    def rows(i, owner, span=None):
        low, high = span or (0, heights[i] // 16)
        return pl.ds(pl.multiple_of(owner * heights[i] + 16 * low, 16), 16 * (high - low))

    def ring(j, step, owner, span=None):
        i, way = PIECES[j]
        part = whole[i].at[way, rows(i, owner, span)]
        return pltpu.make_async_remote_copy(
            src_ref=part, dst_ref=part, send_sem=ring_send.at[step, j], recv_sem=ring_recv.at[step, j],
            device_id=(rep, device(place + 1 if way == 0 else place - 1, core)), device_id_type=MESH,
        )

    def pair(j, step, source, owner, span=None):
        i, way = PIECES[j]
        arrival = CHIPS if span in FIRST[1:] else step
        return pltpu.make_async_remote_copy(
            src_ref=source, dst_ref=whole[i].at[way, rows(i, owner, span)], send_sem=pair_send.at[step, j], recv_sem=pair_recv.at[arrival, j],
            device_id=(rep, 2 * chip + 1 - core), device_id_type=MESH,
        )

    def term(j, step, span=None):
        i, way = PIECES[j]
        owner = device(block(way, step), 1 - core)
        return pair(j, step, g[i].at[0, way, rows(i, owner, span)], owner, span)

    def own(j, step):
        i, way = PIECES[j]
        return pltpu.make_async_copy(g[i].at[0, way, rows(i, device(block(way, step), core))], slots[j], own_sem.at[j])

    def load_w(j):
        i, way = PIECES[j]
        return pltpu.make_async_copy(w[i].at[way, rows(i, me)], slots[j], own_sem.at[j])

    def load_m(j):
        i, way = PIECES[j]
        return pltpu.make_async_copy(m[i].at[way], new_m[i].at[way], m_sem.at[j])

    def load_v(j):
        i, way = PIECES[j]
        return pltpu.make_async_copy(v[i].at[way], new_v[i].at[way], v_sem.at[j])

    def add(j, step, first=False, span=None):
        i, way = PIECES[j]
        groups, columns = tiles(heights[i], whole[i].shape[2])
        mine = pl.multiple_of(device(block(way, step), core) * heights[i], 16)
        other = pl.multiple_of(device(block(way, step), 1 - core) * heights[i], 16)

        def group(r, _):
            for c in columns:
                total = slots[j][pl.ds(r * 16, 16), c].astype(jnp.float32) + whole[i][way, pl.ds(mine + r * 16, 16), c].astype(jnp.float32)
                if not first:
                    total = total + whole[i][way, pl.ds(other + r * 16, 16), c].astype(jnp.float32)
                whole[i][way, pl.ds(other + r * 16, 16), c] = total.astype(jnp.bfloat16)
            return 0

        lax.fori_loop(*(span or (0, groups)), group, 0)

    def last_add(j, so_far):
        i, way = PIECES[j]
        groups, columns = tiles(heights[i], whole[i].shape[2])
        mine = pl.multiple_of(me * heights[i], 16)
        other = pl.multiple_of((2 * chip + 1 - core) * heights[i], 16)

        def group(r, so_far):
            for c in columns:
                total = slots[j][pl.ds(r * 16, 16), c].astype(jnp.float32) + whole[i][way, pl.ds(mine + r * 16, 16), c].astype(jnp.float32)
                total = (total + whole[i][way, pl.ds(other + r * 16, 16), c].astype(jnp.float32)).astype(jnp.bfloat16)
                whole[i][way, pl.ds(mine + r * 16, 16), c] = total
                total = total.astype(jnp.float32)
                total = total * total
                for k in range(0, total.shape[1], 128):
                    so_far = so_far + total[:8, k : k + 128] + total[8:, k : k + 128]
            return so_far

        return lax.fori_loop(0, groups, group, so_far)

    def update(j, factor, span=None):
        i, way = PIECES[j]
        groups, columns = tiles(heights[i], whole[i].shape[2])
        mine = pl.multiple_of(me * heights[i], 16)

        def group(r, _):
            for c in columns:
                here = (way, pl.ds(r * 16, 16), c)
                there = (way, pl.ds(mine + r * 16, 16), c)
                gradient = whole[i][there].astype(jnp.float32) * factor
                new, new_m[i][here], new_v[i][here] = adamw(slots[j][pl.ds(r * 16, 16), c].astype(jnp.float32), new_m[i][here], new_v[i][here], gradient)
                whole[i][there] = new
            return 0

        lax.fori_loop(*(span or (0, groups)), group, 0)

    every = range(len(PIECES))
    for j in every:
        own(j, 0).start()
    barrier = pltpu.get_barrier_semaphore()
    for peer in (2 * chip + 1 - core, device(place + 1, core), device(place - 1, core)):
        pl.semaphore_signal(barrier, inc=1, device_id=(rep, peer), device_id_type=MESH)
    pl.semaphore_wait(barrier, 3)

    for j, span in ORDER:
        term(j, 0, span).start()
    for j, span in ORDER:
        if span not in FIRST[1:]:
            own(j, 0).wait()
        term(j, 0, span).wait_recv()
        add(j, 0, first=True, span=span)
        ring(j, 0, device(block(PIECES[j][1], 0), 1 - core), span).start()
    for j in every:
        term(j, 1).start()
        own(j, 1).start()
    for j in every:
        load_m(j).start()
        load_v(j).start()

    def reduce_step(step, _):
        for j in every:
            term(j, step + 1).start()
        for j in every:
            owner = device(block(PIECES[j][1], step), 1 - core)
            own(j, step).wait()
            term(j, step).wait_recv()
            ring(j, step - 1, owner).wait_recv()
            add(j, step)
            ring(j, step, owner).start()
            own(j, step + 1).start()
            ring(j, step - 1, owner).wait_send()
            term(j, step - 1).wait_send()
        return 0

    lax.fori_loop(1, CHIPS - 1, reduce_step, 0)

    so_far = jnp.zeros((8, 128), jnp.float32)
    for j in every:
        own(j, CHIPS - 1).wait()
        term(j, CHIPS - 1).wait_recv()
        ring(j, CHIPS - 2, 2 * chip + 1 - core).wait_recv()
        so_far = last_add(j, so_far)
        load_w(j).start()
    for j in every:
        term(j, CHIPS - 2).wait_send()
        term(j, CHIPS - 1).wait_send()
        ring(j, CHIPS - 2, 2 * chip + 1 - core).wait_send()

    squares[me] = so_far

    def tell(k):
        return pltpu.make_async_remote_copy(
            src_ref=squares.at[me], dst_ref=squares.at[me], send_sem=sq_send.at[k], recv_sem=sq_recv.at[k],
            device_id=(rep, lax.rem(me + k, DEVICES)), device_id_type=MESH,
        )

    for k in range(1, DEVICES):
        tell(k).start()
    for j in every:
        load_m(j).wait()
        load_v(j).wait()
        load_w(j).wait()
    for k in range(1, DEVICES):
        tell(k).wait_recv()
    total = squares[0]
    for k in range(1, DEVICES):
        total = total + squares[k]
    total = jnp.sum(jnp.sum(total, axis=0, keepdims=True), axis=1, keepdims=True)
    factor = jnp.minimum(1.0, 0.5 * lax.rsqrt(total / count + 1e-30))

    def carried(j, step):
        return device(place - step if PIECES[j][1] == 0 else place + step, core)

    def on(j, step):
        return ring(j, step, carried(j, step))

    def across(j, step):
        i, way = PIECES[j]
        owner = carried(j, step)
        return pair(j, step, whole[i].at[way, rows(i, owner)], owner)

    for j, span in ORDER:
        update(j, factor, span)
        ring(j, 0, me, span).start()
        if span != FIRST[0]:
            across(j, 0).start()

    def gather_step(step, _):
        for j in every:
            on(j, step - 1).wait_recv()
            on(j, step).start()
            across(j, step).start()
            on(j, step - 1).wait_send()
            across(j, step - 1).wait_send()
        return 0

    lax.fori_loop(1, CHIPS - 1, gather_step, 0)
    for j in every:
        on(j, CHIPS - 2).wait_recv()
        across(j, CHIPS - 1).start()
        on(j, CHIPS - 2).wait_send()
        across(j, CHIPS - 2).wait_send()
    for k in range(1, DEVICES):
        tell(k).wait_send()
    for j in every:
        across(j, CHIPS - 1).wait_send()

    def arrived(step, _):
        for j in every:
            across(j, step).wait_recv()
        return 0

    lax.fori_loop(0, CHIPS, arrived, 0)


def put_out(*refs):
    copies = [pltpu.make_async_copy(refs[k].at[layer], refs[9 + k].at[layer], refs[18].at[k, layer]) for k in range(9) for layer in range(2)]
    for copy in copies:
        copy.start()
    for copy in copies:
        copy.wait()


def body(count, *refs):
    groups = [refs[k : k + 3] for k in range(0, 21, 3)]
    kernel(count, *groups, refs[21:23], *refs[23:])


def solution(mesh):
    def step(*arrays):
        weights, moments = arrays[3:6], arrays[6:9]
        count = DEVICES * sum(one.size for one in moments)
        heights = [one.shape[1] for one in moments]
        widths = [one.shape[2] for one in moments]
        dma = pltpu.SemaphoreType.DMA
        out = [pltpu.VMEM(one.shape, jnp.bfloat16) for one in weights] + 2 * [pltpu.VMEM(one.shape, jnp.float32) for one in moments]
        done = pl.pallas_call(
            functools.partial(body, count),
            out_shape=out,
            in_specs=[pl.BlockSpec(memory_space=pltpu.HBM)] * 12,
            out_specs=[pl.BlockSpec(memory_space=pltpu.VMEM)] * 9,
            scratch_shapes=[
                pltpu.VMEM((4, heights[0], widths[0]), jnp.bfloat16),
                pltpu.VMEM((2, heights[2], widths[2]), jnp.bfloat16),
                pltpu.VMEM((DEVICES, 8, 128), jnp.float32),
                dma((6,)), dma((6,)), dma((6,)),
                dma((7, 6)), dma((7, 6)), dma((8, 6)), dma((9, 6)),
                dma((DEVICES,)), dma((DEVICES,)),
            ],
            compiler_params=pltpu.CompilerParams(collective_id=0, has_side_effects=True, vmem_limit_bytes=4 << 20),
            name="train_step",
        )(*arrays)
        return pl.pallas_call(
            put_out,
            out_shape=[jax.ShapeDtypeStruct(one.shape, one.dtype) for one in done],
            in_specs=[pl.BlockSpec(memory_space=pltpu.VMEM)] * 9,
            out_specs=[pl.BlockSpec(memory_space=pltpu.HBM)] * 9,
            scratch_shapes=[dma((9, 2))],
            compiler_params=pltpu.CompilerParams(vmem_limit_bytes=4 << 20),
            name="put_out",
        )(*[pltpu.with_memory_space_constraint(one, pltpu.VMEM) for one in done])

    all_of, cut = P(None, None, None), P(None, "dp", None)
    return jax.shard_map(
        step,
        mesh=mesh,
        in_specs=(P(("rep", "dp"), None, None, None),) * 3 + (all_of,) * 3 + (cut,) * 6,
        out_specs=(P("rep", None, None),) * 3 + (P("rep", "dp", None),) * 6,
        check_vma=False,
    )
```

```python
import functools

import jax
import jax.numpy as jnp
from jax import lax
from jax.experimental import pallas as pl
from jax.experimental.pallas import tpu as pltpu
from jax.sharding import PartitionSpec as P

MESH = pl.DeviceIdType.MESH
CHIPS, DEVICES = 8, 16
FIRST = ((0, 2), (2, 5))
ORDER = [(0, FIRST[0]), (1, FIRST[0]), (0, FIRST[1]), (1, FIRST[1]), (2, None), (3, None), (4, None), (5, None)]
PIECES = [(i, way) for i in range(3) for way in range(2)]


def adamw(w, m, v, g):
    m = 0.9 * m + 0.1 * g
    v = 0.95 * v + 0.05 * g * g
    step = m * lax.rsqrt(v + 1e-8) + 0.1 * w
    return (w - 0.02 * step).astype(jnp.bfloat16), m, v


def at(place):
    return place + lax.div(place, 4) * (11 - 2 * place)


def tiles(height, width):
    wide = 512 if width % 512 == 0 else 640
    return height // 16, [slice(k, k + wide) for k in range(0, width, wide)]


def kernel(count, g, w, m, v, whole, new_m, new_v, last, held, squares, last_sem, own_sem, m_sem, v_sem, ring_send, ring_recv, pair_send, pair_recv, sq_send, sq_recv):
    rep, me = lax.axis_index("rep"), lax.axis_index("dp")
    chip, core = lax.div(me, 2), lax.rem(me, 2)
    place = at(chip)
    heights = [one.shape[1] for one in new_m]
    slots = [held[0].at[0], held[0].at[1], held[0].at[2], held[0].at[3], held[1].at[0], held[1].at[1]]

    def device(place, core):
        return 2 * at(lax.rem(place + 2 * CHIPS, CHIPS)) + core

    def block(way, step):
        return place - 1 - step if way == 0 else place + 1 + step

    def rows(i, owner, span=None):
        low, high = span or (0, heights[i] // 16)
        return pl.ds(pl.multiple_of(owner * heights[i] + 16 * low, 16), 16 * (high - low))

    def ring(j, step, owner, span=None):
        i, way = PIECES[j]
        part = whole[i].at[way, rows(i, owner, span)]
        return pltpu.make_async_remote_copy(
            src_ref=part, dst_ref=part, send_sem=ring_send.at[step, j], recv_sem=ring_recv.at[step, j],
            device_id=(rep, device(place + 1 if way == 0 else place - 1, core)), device_id_type=MESH,
        )

    def pair(j, step, source, owner, span=None):
        i, way = PIECES[j]
        arrival = CHIPS if span in FIRST[1:] else step
        return pltpu.make_async_remote_copy(
            src_ref=source, dst_ref=whole[i].at[way, rows(i, owner, span)], send_sem=pair_send.at[step, j], recv_sem=pair_recv.at[arrival, j],
            device_id=(rep, 2 * chip + 1 - core), device_id_type=MESH,
        )

    def term(j, step, span=None):
        i, way = PIECES[j]
        owner = device(block(way, step), 1 - core)
        return pair(j, step, g[i].at[0, way, rows(i, owner, span)], owner, span)

    def own(j, step):
        i, way = PIECES[j]
        return pltpu.make_async_copy(g[i].at[0, way, rows(i, device(block(way, step), core))], slots[j], own_sem.at[j])

    def load_w(j):
        i, way = PIECES[j]
        return pltpu.make_async_copy(w[i].at[way, rows(i, me)], slots[j], own_sem.at[j])

    def load_m(j):
        i, way = PIECES[j]
        return pltpu.make_async_copy(m[i].at[way], new_m[i].at[way], m_sem.at[j])

    def load_v(j):
        i, way = PIECES[j]
        return pltpu.make_async_copy(v[i].at[way], new_v[i].at[way], v_sem.at[j])

    def add(j, step, first=False, span=None):
        i, way = PIECES[j]
        groups, columns = tiles(heights[i], whole[i].shape[2])
        mine = pl.multiple_of(device(block(way, step), core) * heights[i], 16)
        other = pl.multiple_of(device(block(way, step), 1 - core) * heights[i], 16)

        def group(r, _):
            for c in columns:
                total = slots[j][pl.ds(r * 16, 16), c].astype(jnp.float32) + whole[i][way, pl.ds(mine + r * 16, 16), c].astype(jnp.float32)
                if not first:
                    total = total + whole[i][way, pl.ds(other + r * 16, 16), c].astype(jnp.float32)
                whole[i][way, pl.ds(other + r * 16, 16), c] = total.astype(jnp.bfloat16)
            return 0

        lax.fori_loop(*(span or (0, groups)), group, 0)

    def last_add(j, so_far):
        i, way = PIECES[j]
        groups, columns = tiles(heights[i], whole[i].shape[2])
        mine = pl.multiple_of(me * heights[i], 16)
        other = pl.multiple_of((2 * chip + 1 - core) * heights[i], 16)

        def group(r, so_far):
            for c in columns:
                total = slots[j][pl.ds(r * 16, 16), c].astype(jnp.float32) + whole[i][way, pl.ds(mine + r * 16, 16), c].astype(jnp.float32)
                total = (total + whole[i][way, pl.ds(other + r * 16, 16), c].astype(jnp.float32)).astype(jnp.bfloat16)
                whole[i][way, pl.ds(mine + r * 16, 16), c] = total
                total = total.astype(jnp.float32)
                total = total * total
                for k in range(0, total.shape[1], 128):
                    so_far = so_far + total[:8, k : k + 128] + total[8:, k : k + 128]
            return so_far

        return lax.fori_loop(0, groups, group, so_far)

    def update(j, factor, span=None):
        i, way = PIECES[j]
        groups, columns = tiles(heights[i], whole[i].shape[2])
        mine = pl.multiple_of(me * heights[i], 16)

        def group(r, _):
            for c in columns:
                here = (way, pl.ds(r * 16, 16), c)
                there = (way, pl.ds(mine + r * 16, 16), c)
                gradient = whole[i][there].astype(jnp.float32) * factor
                new, new_m[i][here], new_v[i][here] = adamw(slots[j][pl.ds(r * 16, 16), c].astype(jnp.float32), new_m[i][here], new_v[i][here], gradient)
                whole[i][there] = new
            return 0

        lax.fori_loop(*(span or (0, groups)), group, 0)

    every = range(len(PIECES))
    for j in every:
        own(j, 0).start()
    barrier = pltpu.get_barrier_semaphore()
    for peer in (2 * chip + 1 - core, device(place + 1, core), device(place - 1, core)):
        pl.semaphore_signal(barrier, inc=1, device_id=(rep, peer), device_id_type=MESH)
    pl.semaphore_wait(barrier, 3)

    for j, span in ORDER:
        term(j, 0, span).start()
    for j, span in ORDER:
        if span not in FIRST[1:]:
            own(j, 0).wait()
        term(j, 0, span).wait_recv()
        add(j, 0, first=True, span=span)
        ring(j, 0, device(block(PIECES[j][1], 0), 1 - core), span).start()
    for j in every:
        term(j, 1).start()
        own(j, 1).start()
    for j in every:
        load_m(j).start()
        load_v(j).start()

    def reduce_step(step, _):
        for j in every:
            term(j, step + 1).start()
        for j in every:
            owner = device(block(PIECES[j][1], step), 1 - core)
            own(j, step).wait()
            term(j, step).wait_recv()
            ring(j, step - 1, owner).wait_recv()
            add(j, step)
            ring(j, step, owner).start()
            own(j, step + 1).start()
            ring(j, step - 1, owner).wait_send()
            term(j, step - 1).wait_send()
        return 0

    lax.fori_loop(1, CHIPS - 1, reduce_step, 0)

    so_far = jnp.zeros((8, 128), jnp.float32)
    for j in every:
        own(j, CHIPS - 1).wait()
        term(j, CHIPS - 1).wait_recv()
        ring(j, CHIPS - 2, 2 * chip + 1 - core).wait_recv()
        so_far = last_add(j, so_far)
        load_w(j).start()
    for j in every:
        term(j, CHIPS - 2).wait_send()
        term(j, CHIPS - 1).wait_send()
        ring(j, CHIPS - 2, 2 * chip + 1 - core).wait_send()

    squares[me] = so_far

    def tell(k):
        return pltpu.make_async_remote_copy(
            src_ref=squares.at[me], dst_ref=squares.at[me], send_sem=sq_send.at[k], recv_sem=sq_recv.at[k],
            device_id=(rep, lax.rem(me + k, DEVICES)), device_id_type=MESH,
        )

    for k in range(1, DEVICES):
        tell(k).start()
    for j in every:
        load_m(j).wait()
        load_v(j).wait()
        load_w(j).wait()
    for k in range(1, DEVICES):
        tell(k).wait_recv()
    total = squares[0]
    for k in range(1, DEVICES):
        total = total + squares[k]
    total = jnp.sum(jnp.sum(total, axis=0, keepdims=True), axis=1, keepdims=True)
    factor = jnp.minimum(1.0, 0.5 * lax.rsqrt(total / count + 1e-30))

    def carried(j, step):
        return device(place - step if PIECES[j][1] == 0 else place + step, core)

    def on(j, step):
        return ring(j, step, carried(j, step))

    def across(j, step):
        i, way = PIECES[j]
        owner = carried(j, step)
        return pair(j, step, whole[i].at[way, rows(i, owner)], owner)

    for j, span in ORDER:
        update(j, factor, span)
        ring(j, 0, me, span).start()
        if span != FIRST[0]:
            across(j, 0).start()

    def gather_step(step, _):
        for j in every:
            on(j, step - 1).wait_recv()
            on(j, step).start()
            across(j, step).start()
            on(j, step - 1).wait_send()
            across(j, step - 1).wait_send()
        return 0

    lax.fori_loop(1, CHIPS - 2, gather_step, 0)

    def hand_out(j):
        i, way = PIECES[j]
        return pltpu.make_async_copy(whole[i].at[way, rows(i, carried(j, CHIPS - 2))], last[way].at[i], last_sem.at[j])

    for j in every:
        on(j, CHIPS - 3).wait_recv()
        if j < 4:
            hand_out(j).start()
        else:
            on(j, CHIPS - 2).start()
        across(j, CHIPS - 2).start()
        on(j, CHIPS - 3).wait_send()
        across(j, CHIPS - 3).wait_send()
    for j in every[4:]:
        on(j, CHIPS - 2).wait_recv()
        across(j, CHIPS - 1).start()
        on(j, CHIPS - 2).wait_send()
    for k in range(1, DEVICES):
        tell(k).wait_send()
    for j in every:
        across(j, CHIPS - 2).wait_send()
        if j < 4:
            hand_out(j).wait()
        else:
            across(j, CHIPS - 1).wait_send()
            across(j, CHIPS - 1).wait_recv()

    def arrived(step, _):
        for j in every:
            across(j, step).wait_recv()
        return 0

    lax.fori_loop(0, CHIPS - 1, arrived, 0)


def put_last(*refs):
    arrived, out, sem = refs[2:6], refs[6:8], refs[8]
    me = lax.axis_index("dp")
    chip, core = lax.div(me, 2), lax.rem(me, 2)
    height = arrived[0].shape[1]
    copies = []
    for k, one in enumerate(arrived):
        way = k % 2
        place = lax.rem(at(chip) + (1 if way == 0 else CHIPS - 1), CHIPS)
        owner = 2 * at(place) + (core if k < 2 else 1 - core)
        there = pl.ds(pl.multiple_of(owner * height, 16), height)
        copies += [pltpu.make_async_copy(one.at[i], out[i].at[way, there], sem.at[k, i]) for i in range(2)]
    for copy in copies:
        copy.start()
    for copy in copies:
        copy.wait()


def put_out(*refs):
    copies = [pltpu.make_async_copy(refs[k].at[layer], refs[9 + k].at[layer], refs[18].at[k, layer]) for k in range(9) for layer in range(2)]
    for copy in copies:
        copy.start()
    for copy in copies:
        copy.wait()


def body(count, *refs):
    groups = [refs[k : k + 3] for k in range(0, 21, 3)]
    kernel(count, *groups, refs[21:23], refs[23:25], *refs[25:])


def solution(mesh):
    def step(*arrays):
        weights, moments = arrays[3:6], arrays[6:9]
        count = DEVICES * sum(one.size for one in moments)
        heights = [one.shape[1] for one in moments]
        widths = [one.shape[2] for one in moments]
        dma = pltpu.SemaphoreType.DMA
        out = [pltpu.VMEM(one.shape, jnp.bfloat16) for one in weights] + 2 * [pltpu.VMEM(one.shape, jnp.float32) for one in moments]
        piece = pltpu.HBM((2, *moments[0].shape[1:]), jnp.bfloat16)
        *done, up, down = pl.pallas_call(
            functools.partial(body, count),
            out_shape=[*out, piece, piece],
            in_specs=[pl.BlockSpec(memory_space=pltpu.HBM)] * 12,
            out_specs=[pl.BlockSpec(memory_space=pltpu.VMEM)] * 9 + [pl.BlockSpec(memory_space=pltpu.HBM)] * 2,
            scratch_shapes=[
                pltpu.VMEM((4, heights[0], widths[0]), jnp.bfloat16),
                pltpu.VMEM((2, heights[2], widths[2]), jnp.bfloat16),
                pltpu.VMEM((DEVICES, 8, 128), jnp.float32),
                dma((4,)), dma((6,)), dma((6,)), dma((6,)),
                dma((7, 6)), dma((7, 6)), dma((8, 6)), dma((9, 6)),
                dma((DEVICES,)), dma((DEVICES,)),
            ],
            compiler_params=pltpu.CompilerParams(collective_id=0, has_side_effects=True, vmem_limit_bytes=4 << 20),
            name="train_step",
        )(*arrays)
        ring = [place + place // 4 * (11 - 2 * place) for place in range(CHIPS)]
        hop = [(2 * ring[k] + core, 2 * ring[(k + 1) % CHIPS] + core) for k in range(CHIPS) for core in range(2)]
        up = lax.ppermute(up, "dp", hop)
        down = lax.ppermute(down, "dp", [(b, a) for a, b in hop])
        in_hbm, in_vmem = pl.BlockSpec(memory_space=pltpu.HBM), pl.BlockSpec(memory_space=pltpu.VMEM)
        gate, up_w, *rest = pl.pallas_call(
            put_out,
            out_shape=[jax.ShapeDtypeStruct(one.shape, one.dtype) for one in done],
            in_specs=[in_vmem] * 9,
            out_specs=[in_hbm] * 9,
            scratch_shapes=[dma((9, 2))],
            compiler_params=pltpu.CompilerParams(vmem_limit_bytes=4 << 20),
            cost_estimate=pl.CostEstimate(flops=500_000_000, bytes_accessed=60_000_000, transcendentals=0),
            name="put_out",
        )(*[pltpu.with_memory_space_constraint(one, pltpu.VMEM) for one in done])
        up, down, rest[-1] = lax.optimization_barrier((up, down, rest[-1]))
        partner = [(k, k + 1 - 2 * (k % 2)) for k in range(DEVICES)]
        across = [lax.ppermute(one, "dp", partner) for one in (up, down)]
        gate, up_w = pl.pallas_call(
            put_last,
            out_shape=[jax.ShapeDtypeStruct(one.shape, one.dtype) for one in (gate, up_w)],
            in_specs=[in_hbm] * 2 + [in_vmem] * 4,
            out_specs=[in_hbm] * 2,
            scratch_shapes=[dma((4, 2))],
            input_output_aliases={0: 0, 1: 1},
            compiler_params=pltpu.CompilerParams(vmem_limit_bytes=16 << 20),
            name="put_last",
        )(gate, up_w, up, down, *across)
        return (gate, up_w, *rest)

    all_of, cut = P(None, None, None), P(None, "dp", None)
    return jax.shard_map(
        step,
        mesh=mesh,
        in_specs=(P(("rep", "dp"), None, None, None),) * 3 + (all_of,) * 3 + (cut,) * 6,
        out_specs=(P("rep", None, None),) * 3 + (P("rep", "dp", None),) * 6,
        check_vma=False,
    )
```

```python
import functools

import jax
import jax.numpy as jnp
from jax import lax
from jax.experimental import pallas as pl
from jax.experimental.pallas import tpu as pltpu
from jax.sharding import PartitionSpec as P

MESH = pl.DeviceIdType.MESH
CHIPS, DEVICES = 8, 16
FIRST = ((0, 2), (2, 5))
ORDER = [(0, FIRST[0]), (1, FIRST[0]), (0, FIRST[1]), (1, FIRST[1]), (2, None), (3, None), (4, None), (5, None)]
PIECES = [(i, way) for i in range(3) for way in range(2)]


def adamw(w, m, v, g):
    m = 0.9 * m + 0.1 * g
    v = 0.95 * v + 0.05 * g * g
    step = m * lax.rsqrt(v + 1e-8) + 0.1 * w
    return (w - 0.02 * step).astype(jnp.bfloat16), m, v


def at(place):
    return place + lax.div(place, 4) * (11 - 2 * place)


def tiles(height, width):
    wide = 512 if width % 512 == 0 else 640
    return height // 16, [slice(k, k + wide) for k in range(0, width, wide)]


def kernel(count, g, w, m, v, whole, new_m, new_v, last, held, squares, last_sem, own_sem, m_sem, v_sem, ring_send, ring_recv, pair_send, pair_recv, sq_send, sq_recv):
    rep, me = lax.axis_index("rep"), lax.axis_index("dp")
    chip, core = lax.div(me, 2), lax.rem(me, 2)
    place = at(chip)
    heights = [one.shape[1] for one in new_m]
    slots = [held[0].at[0], held[0].at[1], held[0].at[2], held[0].at[3], held[1].at[0], held[1].at[1]]

    def device(place, core):
        return 2 * at(lax.rem(place + 2 * CHIPS, CHIPS)) + core

    def block(way, step):
        return place - 1 - step if way == 0 else place + 1 + step

    def rows(i, owner, span=None):
        low, high = span or (0, heights[i] // 16)
        return pl.ds(pl.multiple_of(owner * heights[i] + 16 * low, 16), 16 * (high - low))

    def ring(j, step, owner, span=None):
        i, way = PIECES[j]
        part = whole[i].at[way, rows(i, owner, span)]
        return pltpu.make_async_remote_copy(
            src_ref=part, dst_ref=part, send_sem=ring_send.at[step, j], recv_sem=ring_recv.at[step, j],
            device_id=(rep, device(place + 1 if way == 0 else place - 1, core)), device_id_type=MESH,
        )

    def pair(j, step, source, owner, span=None):
        i, way = PIECES[j]
        arrival = CHIPS if span in FIRST[1:] else step
        return pltpu.make_async_remote_copy(
            src_ref=source, dst_ref=whole[i].at[way, rows(i, owner, span)], send_sem=pair_send.at[step, j], recv_sem=pair_recv.at[arrival, j],
            device_id=(rep, 2 * chip + 1 - core), device_id_type=MESH,
        )

    def term(j, step, span=None):
        i, way = PIECES[j]
        owner = device(block(way, step), 1 - core)
        return pair(j, step, g[i].at[0, way, rows(i, owner, span)], owner, span)

    def own(j, step):
        i, way = PIECES[j]
        return pltpu.make_async_copy(g[i].at[0, way, rows(i, device(block(way, step), core))], slots[j], own_sem.at[j])

    def load_w(j):
        i, way = PIECES[j]
        return pltpu.make_async_copy(w[i].at[way, rows(i, me)], slots[j], own_sem.at[j])

    def load_m(j):
        i, way = PIECES[j]
        return pltpu.make_async_copy(m[i].at[way], new_m[i].at[way], m_sem.at[j])

    def load_v(j):
        i, way = PIECES[j]
        return pltpu.make_async_copy(v[i].at[way], new_v[i].at[way], v_sem.at[j])

    def add(j, step, first=False, span=None):
        i, way = PIECES[j]
        groups, columns = tiles(heights[i], whole[i].shape[2])
        mine = pl.multiple_of(device(block(way, step), core) * heights[i], 16)
        other = pl.multiple_of(device(block(way, step), 1 - core) * heights[i], 16)

        def group(r, _):
            for c in columns:
                total = slots[j][pl.ds(r * 16, 16), c].astype(jnp.float32) + whole[i][way, pl.ds(mine + r * 16, 16), c].astype(jnp.float32)
                if not first:
                    total = total + whole[i][way, pl.ds(other + r * 16, 16), c].astype(jnp.float32)
                whole[i][way, pl.ds(other + r * 16, 16), c] = total.astype(jnp.bfloat16)
            return 0

        lax.fori_loop(*(span or (0, groups)), group, 0)

    def last_add(j, so_far):
        i, way = PIECES[j]
        groups, columns = tiles(heights[i], whole[i].shape[2])
        mine = pl.multiple_of(me * heights[i], 16)
        other = pl.multiple_of((2 * chip + 1 - core) * heights[i], 16)

        def group(r, so_far):
            for c in columns:
                total = slots[j][pl.ds(r * 16, 16), c].astype(jnp.float32) + whole[i][way, pl.ds(mine + r * 16, 16), c].astype(jnp.float32)
                total = (total + whole[i][way, pl.ds(other + r * 16, 16), c].astype(jnp.float32)).astype(jnp.bfloat16)
                whole[i][way, pl.ds(mine + r * 16, 16), c] = total
                total = total.astype(jnp.float32)
                total = total * total
                for k in range(0, total.shape[1], 128):
                    so_far = so_far + total[:8, k : k + 128] + total[8:, k : k + 128]
            return so_far

        return lax.fori_loop(0, groups, group, so_far)

    def update(j, factor, span=None):
        i, way = PIECES[j]
        groups, columns = tiles(heights[i], whole[i].shape[2])
        mine = pl.multiple_of(me * heights[i], 16)

        def group(r, _):
            for c in columns:
                here = (way, pl.ds(r * 16, 16), c)
                there = (way, pl.ds(mine + r * 16, 16), c)
                gradient = whole[i][there].astype(jnp.float32) * factor
                new, new_m[i][here], new_v[i][here] = adamw(slots[j][pl.ds(r * 16, 16), c].astype(jnp.float32), new_m[i][here], new_v[i][here], gradient)
                whole[i][there] = new
            return 0

        lax.fori_loop(*(span or (0, groups)), group, 0)

    every = range(len(PIECES))
    for j in every:
        own(j, 0).start()
    barrier = pltpu.get_barrier_semaphore()
    for peer in (2 * chip + 1 - core, device(place + 1, core), device(place - 1, core)):
        pl.semaphore_signal(barrier, inc=1, device_id=(rep, peer), device_id_type=MESH)
    pl.semaphore_wait(barrier, 3)

    for j, span in ORDER:
        term(j, 0, span).start()
    for j, span in ORDER:
        if span not in FIRST[1:]:
            own(j, 0).wait()
        term(j, 0, span).wait_recv()
        add(j, 0, first=True, span=span)
        ring(j, 0, device(block(PIECES[j][1], 0), 1 - core), span).start()
    for j in every:
        term(j, 1).start()
        own(j, 1).start()
    for j in every:
        load_m(j).start()
        load_v(j).start()

    def reduce_step(step, _):
        for j in every:
            term(j, step + 1).start()
        for j in every:
            owner = device(block(PIECES[j][1], step), 1 - core)
            own(j, step).wait()
            term(j, step).wait_recv()
            ring(j, step - 1, owner).wait_recv()
            add(j, step)
            ring(j, step, owner).start()
            own(j, step + 1).start()
            ring(j, step - 1, owner).wait_send()
            term(j, step - 1).wait_send()
        return 0

    lax.fori_loop(1, CHIPS - 1, reduce_step, 0)

    so_far = jnp.zeros((8, 128), jnp.float32)
    for j in every:
        own(j, CHIPS - 1).wait()
        term(j, CHIPS - 1).wait_recv()
        term(j, CHIPS - 2).wait_send()
        term(j, CHIPS - 1).wait_send()
        ring(j, CHIPS - 2, 2 * chip + 1 - core).wait_recv()
        so_far = last_add(j, so_far)
        load_w(j).start()
    for j in every:
        ring(j, CHIPS - 2, 2 * chip + 1 - core).wait_send()

    squares[me] = so_far

    def tell(k):
        return pltpu.make_async_remote_copy(
            src_ref=squares.at[me], dst_ref=squares.at[me], send_sem=sq_send.at[k], recv_sem=sq_recv.at[k],
            device_id=(rep, lax.rem(me + k, DEVICES)), device_id_type=MESH,
        )

    for k in range(1, DEVICES):
        tell(k).start()
    for j in every:
        load_m(j).wait()
        load_v(j).wait()
        load_w(j).wait()
    for k in range(1, DEVICES):
        tell(k).wait_recv()
    total = squares[0]
    for k in range(1, DEVICES):
        total = total + squares[k]
    total = jnp.sum(jnp.sum(total, axis=0, keepdims=True), axis=1, keepdims=True)
    factor = jnp.minimum(1.0, 0.5 * lax.rsqrt(total / count + 1e-30))

    def carried(j, step):
        return device(place - step if PIECES[j][1] == 0 else place + step, core)

    def on(j, step):
        return ring(j, step, carried(j, step))

    def across(j, step):
        i, way = PIECES[j]
        owner = carried(j, step)
        return pair(j, step, whole[i].at[way, rows(i, owner)], owner)

    for j, span in ORDER:
        update(j, factor, span)
        ring(j, 0, me, span).start()
        if span != FIRST[0]:
            across(j, 0).start()

    for k in range(1, DEVICES):
        tell(k).wait_send()

    def gather_step(step, _):
        for j in every:
            on(j, step - 1).wait_recv()
            on(j, step).start()
            across(j, step).start()
            on(j, step - 1).wait_send()
            across(j, step - 1).wait_send()
            across(j, step - 1).wait_recv()
        return 0

    lax.fori_loop(1, CHIPS - 2, gather_step, 0)

    def hand_out(j):
        i, way = PIECES[j]
        return pltpu.make_async_copy(whole[i].at[way, rows(i, carried(j, CHIPS - 2))], last[j], last_sem.at[j])

    for j in every:
        on(j, CHIPS - 3).wait_recv()
        if j < 4:
            hand_out(j).start()
        else:
            on(j, CHIPS - 2).start()
        across(j, CHIPS - 2).start()
        on(j, CHIPS - 3).wait_send()
        across(j, CHIPS - 3).wait_send()
        across(j, CHIPS - 3).wait_recv()
    for j in every[4:]:
        on(j, CHIPS - 2).wait_recv()
        across(j, CHIPS - 1).start()
        on(j, CHIPS - 2).wait_send()
    for j in every:
        across(j, CHIPS - 2).wait_send()
        across(j, CHIPS - 2).wait_recv()
        if j < 4:
            hand_out(j).wait()
    for j in every[4:]:
        across(j, CHIPS - 1).wait_send()
        across(j, CHIPS - 1).wait_recv()


def put_last(*refs):
    arrived, out, sem = refs[2:10], refs[10:12], refs[12]
    me = lax.axis_index("dp")
    chip, core = lax.div(me, 2), lax.rem(me, 2)
    height = arrived[0].shape[0]
    copies = []
    for k, one in enumerate(arrived):
        i, way = PIECES[k % 4]
        place = lax.rem(at(chip) + (1 if way == 0 else CHIPS - 1), CHIPS)
        owner = 2 * at(place) + (core if k < 4 else 1 - core)
        there = pl.ds(pl.multiple_of(owner * height, 16), height)
        copies.append(pltpu.make_async_copy(one, out[i].at[way, there], sem.at[k]))
    for copy in copies:
        copy.start()
    for copy in copies:
        copy.wait()


def put_out(*refs):
    copies = [pltpu.make_async_copy(refs[k].at[layer], refs[9 + k].at[layer], refs[18].at[k, layer]) for k in range(9) for layer in range(2)]
    for copy in copies:
        copy.start()
    for copy in copies:
        copy.wait()


def body(count, *refs):
    groups = [refs[k : k + 3] for k in range(0, 21, 3)]
    kernel(count, *groups, refs[21:25], refs[25:27], *refs[27:])


def solution(mesh):
    def step(*arrays):
        weights, moments = arrays[3:6], arrays[6:9]
        count = DEVICES * sum(one.size for one in moments)
        heights = [one.shape[1] for one in moments]
        widths = [one.shape[2] for one in moments]
        dma = pltpu.SemaphoreType.DMA
        out = [pltpu.VMEM(one.shape, jnp.bfloat16) for one in weights] + 2 * [pltpu.VMEM(one.shape, jnp.float32) for one in moments]
        piece = pltpu.HBM(moments[0].shape[1:], jnp.bfloat16)
        *done, gate0, gate1, up0, up1 = pl.pallas_call(
            functools.partial(body, count),
            out_shape=[*out, piece, piece, piece, piece],
            in_specs=[pl.BlockSpec(memory_space=pltpu.HBM)] * 12,
            out_specs=[pl.BlockSpec(memory_space=pltpu.VMEM)] * 9 + [pl.BlockSpec(memory_space=pltpu.HBM)] * 4,
            scratch_shapes=[
                pltpu.VMEM((4, heights[0], widths[0]), jnp.bfloat16),
                pltpu.VMEM((2, heights[2], widths[2]), jnp.bfloat16),
                pltpu.VMEM((DEVICES, 8, 128), jnp.float32),
                dma((4,)), dma((6,)), dma((6,)), dma((6,)),
                dma((7, 6)), dma((7, 6)), dma((8, 6)), dma((9, 6)),
                dma((DEVICES,)), dma((DEVICES,)),
            ],
            compiler_params=pltpu.CompilerParams(collective_id=0, has_side_effects=True, vmem_limit_bytes=4 << 20),
            name="train_step",
        )(*arrays)
        ring = [place + place // 4 * (11 - 2 * place) for place in range(CHIPS)]
        hop = [(2 * ring[k] + core, 2 * ring[(k + 1) % CHIPS] + core) for k in range(CHIPS) for core in range(2)]
        back = [(b, a) for a, b in hop]
        last = [lax.ppermute(one, "dp", way) for one, way in ((gate0, hop), (gate1, back), (up0, hop), (up1, back))]
        in_hbm, in_vmem = pl.BlockSpec(memory_space=pltpu.HBM), pl.BlockSpec(memory_space=pltpu.VMEM)
        gate, up_w, *rest = pl.pallas_call(
            put_out,
            out_shape=[jax.ShapeDtypeStruct(one.shape, one.dtype) for one in done],
            in_specs=[in_vmem] * 9,
            out_specs=[in_hbm] * 9,
            scratch_shapes=[dma((9, 2))],
            compiler_params=pltpu.CompilerParams(vmem_limit_bytes=4 << 20),
            cost_estimate=pl.CostEstimate(flops=500_000_000, bytes_accessed=60_000_000, transcendentals=0),
            name="put_out",
        )(*[pltpu.with_memory_space_constraint(one, pltpu.VMEM) for one in done])
        last[0], last[1], rest[-1] = lax.optimization_barrier((last[0], last[1], rest[-1]))
        last[2], last[3], rest[-2] = lax.optimization_barrier((last[2], last[3], rest[-2]))
        partner = [(k, k + 1 - 2 * (k % 2)) for k in range(DEVICES)]
        across = [lax.ppermute(one, "dp", partner) for one in last]
        gate, up_w = pl.pallas_call(
            put_last,
            out_shape=[jax.ShapeDtypeStruct(one.shape, one.dtype) for one in (gate, up_w)],
            in_specs=[in_hbm] * 2 + [in_vmem] * 8,
            out_specs=[in_hbm] * 2,
            scratch_shapes=[dma((8,))],
            input_output_aliases={0: 0, 1: 1},
            compiler_params=pltpu.CompilerParams(vmem_limit_bytes=16 << 20),
            name="put_last",
        )(gate, up_w, *last, *across)
        return (gate, up_w, *rest)

    all_of, cut = P(None, None, None), P(None, "dp", None)
    return jax.shard_map(
        step,
        mesh=mesh,
        in_specs=(P(("rep", "dp"), None, None, None),) * 3 + (all_of,) * 3 + (cut,) * 6,
        out_specs=(P("rep", None, None),) * 3 + (P("rep", "dp", None),) * 6,
        check_vma=False,
    )
```

```python
import functools

import jax
import jax.numpy as jnp
from jax import lax
from jax.experimental import pallas as pl
from jax.experimental.pallas import tpu as pltpu
from jax.sharding import PartitionSpec as P

MESH = pl.DeviceIdType.MESH
CHIPS, DEVICES = 8, 16
FIRST = ((0, 1), (1, 5))
ORDER = [(0, FIRST[0]), (1, FIRST[0]), (0, FIRST[1]), (1, FIRST[1]), (2, None), (3, None), (4, None), (5, None)]
PIECES = [(i, way) for i in range(3) for way in range(2)]


def adamw(w, m, v, g):
    m = 0.9 * m + 0.1 * g
    v = 0.95 * v + 0.05 * g * g
    step = m * lax.rsqrt(v + 1e-8) + 0.1 * w
    return (w - 0.02 * step).astype(jnp.bfloat16), m, v


def at(place):
    return place + lax.div(place, 4) * (11 - 2 * place)


def tiles(height, width):
    wide = 512 if width % 512 == 0 else 640
    return height // 16, [slice(k, k + wide) for k in range(0, width, wide)]


def kernel(count, g, w, m, v, whole, new_m, new_v, last, held, squares, last_sem, own_sem, m_sem, v_sem, ring_send, ring_recv, pair_send, pair_recv, sq_send, sq_recv):
    rep, me = lax.axis_index("rep"), lax.axis_index("dp")
    chip, core = lax.div(me, 2), lax.rem(me, 2)
    place = at(chip)
    heights = [one.shape[1] for one in new_m]
    slots = [held[0].at[0], held[0].at[1], held[0].at[2], held[0].at[3], held[1].at[0], held[1].at[1]]

    def device(place, core):
        return 2 * at(lax.rem(place + 2 * CHIPS, CHIPS)) + core

    def block(way, step):
        return place - 1 - step if way == 0 else place + 1 + step

    def rows(i, owner, span=None):
        low, high = span or (0, heights[i] // 16)
        return pl.ds(pl.multiple_of(owner * heights[i] + 16 * low, 16), 16 * (high - low))

    def ring(j, step, owner, span=None):
        i, way = PIECES[j]
        part = whole[i].at[way, rows(i, owner, span)]
        return pltpu.make_async_remote_copy(
            src_ref=part, dst_ref=part, send_sem=ring_send.at[step, j], recv_sem=ring_recv.at[step, j],
            device_id=(rep, device(place + 1 if way == 0 else place - 1, core)), device_id_type=MESH,
        )

    def pair(j, step, source, owner, span=None):
        i, way = PIECES[j]
        arrival = CHIPS if span in FIRST[1:] else step
        return pltpu.make_async_remote_copy(
            src_ref=source, dst_ref=whole[i].at[way, rows(i, owner, span)], send_sem=pair_send.at[step, j], recv_sem=pair_recv.at[arrival, j],
            device_id=(rep, 2 * chip + 1 - core), device_id_type=MESH,
        )

    def term(j, step, span=None):
        i, way = PIECES[j]
        owner = device(block(way, step), 1 - core)
        return pair(j, step, g[i].at[0, way, rows(i, owner, span)], owner, span)

    def own(j, step):
        i, way = PIECES[j]
        return pltpu.make_async_copy(g[i].at[0, way, rows(i, device(block(way, step), core))], slots[j], own_sem.at[j])

    def load_w(j):
        i, way = PIECES[j]
        return pltpu.make_async_copy(w[i].at[way, rows(i, me)], slots[j], own_sem.at[j])

    def load_m(j):
        i, way = PIECES[j]
        return pltpu.make_async_copy(m[i].at[way], new_m[i].at[way], m_sem.at[j])

    def load_v(j):
        i, way = PIECES[j]
        return pltpu.make_async_copy(v[i].at[way], new_v[i].at[way], v_sem.at[j])

    def add(j, step, first=False, span=None):
        i, way = PIECES[j]
        groups, columns = tiles(heights[i], whole[i].shape[2])
        mine = pl.multiple_of(device(block(way, step), core) * heights[i], 16)
        other = pl.multiple_of(device(block(way, step), 1 - core) * heights[i], 16)

        def group(r, _):
            for c in columns:
                total = slots[j][pl.ds(r * 16, 16), c].astype(jnp.float32) + whole[i][way, pl.ds(mine + r * 16, 16), c].astype(jnp.float32)
                if not first:
                    total = total + whole[i][way, pl.ds(other + r * 16, 16), c].astype(jnp.float32)
                whole[i][way, pl.ds(other + r * 16, 16), c] = total.astype(jnp.bfloat16)
            return 0

        lax.fori_loop(*(span or (0, groups)), group, 0)

    def last_add(j, so_far):
        i, way = PIECES[j]
        groups, columns = tiles(heights[i], whole[i].shape[2])
        mine = pl.multiple_of(me * heights[i], 16)
        other = pl.multiple_of((2 * chip + 1 - core) * heights[i], 16)

        def group(r, so_far):
            for c in columns:
                total = slots[j][pl.ds(r * 16, 16), c].astype(jnp.float32) + whole[i][way, pl.ds(mine + r * 16, 16), c].astype(jnp.float32)
                total = (total + whole[i][way, pl.ds(other + r * 16, 16), c].astype(jnp.float32)).astype(jnp.bfloat16)
                whole[i][way, pl.ds(mine + r * 16, 16), c] = total
                total = total.astype(jnp.float32)
                total = total * total
                for k in range(0, total.shape[1], 128):
                    so_far = so_far + total[:8, k : k + 128] + total[8:, k : k + 128]
            return so_far

        return lax.fori_loop(0, groups, group, so_far)

    def update(j, factor, span=None):
        i, way = PIECES[j]
        groups, columns = tiles(heights[i], whole[i].shape[2])
        mine = pl.multiple_of(me * heights[i], 16)

        def group(r, _):
            for c in columns:
                here = (way, pl.ds(r * 16, 16), c)
                there = (way, pl.ds(mine + r * 16, 16), c)
                gradient = whole[i][there].astype(jnp.float32) * factor
                new, new_m[i][here], new_v[i][here] = adamw(slots[j][pl.ds(r * 16, 16), c].astype(jnp.float32), new_m[i][here], new_v[i][here], gradient)
                whole[i][there] = new
            return 0

        lax.fori_loop(*(span or (0, groups)), group, 0)

    every = range(len(PIECES))
    for j in every:
        own(j, 0).start()
    barrier = pltpu.get_barrier_semaphore()
    for peer in (2 * chip + 1 - core, device(place + 1, core), device(place - 1, core)):
        pl.semaphore_signal(barrier, inc=1, device_id=(rep, peer), device_id_type=MESH)
    pl.semaphore_wait(barrier, 3)

    for j, span in ORDER:
        term(j, 0, span).start()
    for j, span in ORDER:
        if span not in FIRST[1:]:
            own(j, 0).wait()
        term(j, 0, span).wait_recv()
        add(j, 0, first=True, span=span)
        ring(j, 0, device(block(PIECES[j][1], 0), 1 - core), span).start()
    for j in every:
        term(j, 1).start()
        own(j, 1).start()
    for j in every:
        load_m(j).start()
        load_v(j).start()

    def reduce_step(step, _):
        for j in every:
            term(j, step + 1).start()
        for j in every:
            owner = device(block(PIECES[j][1], step), 1 - core)
            own(j, step).wait()
            term(j, step).wait_recv()
            ring(j, step - 1, owner).wait_recv()
            add(j, step)
            ring(j, step, owner).start()
            own(j, step + 1).start()
            ring(j, step - 1, owner).wait_send()
            term(j, step - 1).wait_send()
        return 0

    lax.fori_loop(1, CHIPS - 1, reduce_step, 0)

    so_far = jnp.zeros((8, 128), jnp.float32)
    for j in every:
        own(j, CHIPS - 1).wait()
        term(j, CHIPS - 1).wait_recv()
        term(j, CHIPS - 2).wait_send()
        term(j, CHIPS - 1).wait_send()
        ring(j, CHIPS - 2, 2 * chip + 1 - core).wait_recv()
        so_far = last_add(j, so_far)
        load_w(j).start()
    for j in every:
        ring(j, CHIPS - 2, 2 * chip + 1 - core).wait_send()

    squares[me] = so_far

    def tell(k):
        return pltpu.make_async_remote_copy(
            src_ref=squares.at[me], dst_ref=squares.at[me], send_sem=sq_send.at[k], recv_sem=sq_recv.at[k],
            device_id=(rep, lax.rem(me + k, DEVICES)), device_id_type=MESH,
        )

    for k in range(1, DEVICES):
        tell(k).start()
    for j in every:
        load_m(j).wait()
        load_v(j).wait()
        load_w(j).wait()
    for k in range(1, DEVICES):
        tell(k).wait_recv()
    total = squares[0]
    for k in range(1, DEVICES):
        total = total + squares[k]
    total = jnp.sum(jnp.sum(total, axis=0, keepdims=True), axis=1, keepdims=True)
    factor = jnp.minimum(1.0, 0.5 * lax.rsqrt(total / count + 1e-30))

    def carried(j, step):
        return device(place - step if PIECES[j][1] == 0 else place + step, core)

    def on(j, step):
        return ring(j, step, carried(j, step))

    def across(j, step):
        i, way = PIECES[j]
        owner = carried(j, step)
        return pair(j, step, whole[i].at[way, rows(i, owner)], owner)

    for j, span in ORDER:
        update(j, factor, span)
        ring(j, 0, me, span).start()
        if span != FIRST[0]:
            across(j, 0).start()

    for k in range(1, DEVICES):
        tell(k).wait_send()

    def gather_step(step, _):
        for j in every:
            on(j, step - 1).wait_recv()
            on(j, step).start()
            across(j, step).start()
            on(j, step - 1).wait_send()
            across(j, step - 1).wait_send()
            across(j, step - 1).wait_recv()
        return 0

    lax.fori_loop(1, CHIPS - 2, gather_step, 0)

    def hand_out(j):
        i, way = PIECES[j]
        return pltpu.make_async_copy(whole[i].at[way, rows(i, carried(j, CHIPS - 2))], last[j], last_sem.at[j])

    for j in every:
        on(j, CHIPS - 3).wait_recv()
        if j < 4:
            hand_out(j).start()
        else:
            on(j, CHIPS - 2).start()
        across(j, CHIPS - 2).start()
        on(j, CHIPS - 3).wait_send()
        across(j, CHIPS - 3).wait_send()
        across(j, CHIPS - 3).wait_recv()
    for j in every[4:]:
        on(j, CHIPS - 2).wait_recv()
        across(j, CHIPS - 1).start()
        on(j, CHIPS - 2).wait_send()
    for j in every:
        across(j, CHIPS - 2).wait_send()
        across(j, CHIPS - 2).wait_recv()
        if j < 4:
            hand_out(j).wait()
    for j in every[4:]:
        across(j, CHIPS - 1).wait_send()
        across(j, CHIPS - 1).wait_recv()


def put_last(*refs):
    arrived, out, sem = refs[2:10], refs[10:12], refs[12]
    me = lax.axis_index("dp")
    chip, core = lax.div(me, 2), lax.rem(me, 2)
    height = arrived[0].shape[0]
    copies = []
    for k, one in enumerate(arrived):
        i, way = PIECES[k % 4]
        place = lax.rem(at(chip) + (1 if way == 0 else CHIPS - 1), CHIPS)
        owner = 2 * at(place) + (core if k < 4 else 1 - core)
        there = pl.ds(pl.multiple_of(owner * height, 16), height)
        copies.append(pltpu.make_async_copy(one, out[i].at[way, there], sem.at[k]))
    for copy in copies:
        copy.start()
    for copy in copies:
        copy.wait()


def put_out(*refs):
    copies = [pltpu.make_async_copy(refs[k].at[layer], refs[9 + k].at[layer], refs[18].at[k, layer]) for k in range(9) for layer in range(2)]
    for copy in copies:
        copy.start()
    for copy in copies:
        copy.wait()


def body(count, *refs):
    groups = [refs[k : k + 3] for k in range(0, 21, 3)]
    kernel(count, *groups, refs[21:25], refs[25:27], *refs[27:])


def solution(mesh):
    def step(*arrays):
        weights, moments = arrays[3:6], arrays[6:9]
        count = DEVICES * sum(one.size for one in moments)
        heights = [one.shape[1] for one in moments]
        widths = [one.shape[2] for one in moments]
        dma = pltpu.SemaphoreType.DMA
        out = [pltpu.VMEM(one.shape, jnp.bfloat16) for one in weights] + 2 * [pltpu.VMEM(one.shape, jnp.float32) for one in moments]
        piece = pltpu.HBM(moments[0].shape[1:], jnp.bfloat16)
        *done, gate0, gate1, up0, up1 = pl.pallas_call(
            functools.partial(body, count),
            out_shape=[*out, piece, piece, piece, piece],
            in_specs=[pl.BlockSpec(memory_space=pltpu.HBM)] * 12,
            out_specs=[pl.BlockSpec(memory_space=pltpu.VMEM)] * 9 + [pl.BlockSpec(memory_space=pltpu.HBM)] * 4,
            scratch_shapes=[
                pltpu.VMEM((4, heights[0], widths[0]), jnp.bfloat16),
                pltpu.VMEM((2, heights[2], widths[2]), jnp.bfloat16),
                pltpu.VMEM((DEVICES, 8, 128), jnp.float32),
                dma((4,)), dma((6,)), dma((6,)), dma((6,)),
                dma((7, 6)), dma((7, 6)), dma((8, 6)), dma((9, 6)),
                dma((DEVICES,)), dma((DEVICES,)),
            ],
            compiler_params=pltpu.CompilerParams(collective_id=0, has_side_effects=True, vmem_limit_bytes=4 << 20),
            name="train_step",
        )(*arrays)
        ring = [place + place // 4 * (11 - 2 * place) for place in range(CHIPS)]
        hop = [(2 * ring[k] + core, 2 * ring[(k + 1) % CHIPS] + core) for k in range(CHIPS) for core in range(2)]
        back = [(b, a) for a, b in hop]
        last = [lax.ppermute(one, "dp", way) for one, way in ((gate0, hop), (gate1, back), (up0, hop), (up1, back))]
        in_hbm, in_vmem = pl.BlockSpec(memory_space=pltpu.HBM), pl.BlockSpec(memory_space=pltpu.VMEM)
        gate, up_w, *rest = pl.pallas_call(
            put_out,
            out_shape=[jax.ShapeDtypeStruct(one.shape, one.dtype) for one in done],
            in_specs=[in_vmem] * 9,
            out_specs=[in_hbm] * 9,
            scratch_shapes=[dma((9, 2))],
            compiler_params=pltpu.CompilerParams(vmem_limit_bytes=4 << 20),
            cost_estimate=pl.CostEstimate(flops=500_000_000, bytes_accessed=60_000_000, transcendentals=0),
            name="put_out",
        )(*[pltpu.with_memory_space_constraint(one, pltpu.VMEM) for one in done])
        last[0], last[1], rest[-1] = lax.optimization_barrier((last[0], last[1], rest[-1]))
        last[2], last[3], rest[-2] = lax.optimization_barrier((last[2], last[3], rest[-2]))
        partner = [(k, k + 1 - 2 * (k % 2)) for k in range(DEVICES)]
        across = [lax.ppermute(one, "dp", partner) for one in last]
        gate, up_w = pl.pallas_call(
            put_last,
            out_shape=[jax.ShapeDtypeStruct(one.shape, one.dtype) for one in (gate, up_w)],
            in_specs=[in_hbm] * 2 + [in_vmem] * 8,
            out_specs=[in_hbm] * 2,
            scratch_shapes=[dma((8,))],
            input_output_aliases={0: 0, 1: 1},
            compiler_params=pltpu.CompilerParams(vmem_limit_bytes=16 << 20),
            name="put_last",
        )(gate, up_w, *last, *across)
        return (gate, up_w, *rest)

    all_of, cut = P(None, None, None), P(None, "dp", None)
    return jax.shard_map(
        step,
        mesh=mesh,
        in_specs=(P(("rep", "dp"), None, None, None),) * 3 + (all_of,) * 3 + (cut,) * 6,
        out_specs=(P("rep", None, None),) * 3 + (P("rep", "dp", None),) * 6,
        check_vma=False,
    )
```
